32 devices in a mesh: dp: 8 (over z, y), mp: 4 (over x, core).
Axes of the slice: x: 2, y: 2, z: 4, core: 2. Of those that a mesh axis runs over, the one named last changes fastest.
Arguments:
- grads: bfloat16 [8, 8, 128, 128], P('dp', None, 'mp'), may hold values from -24 to 24
- weights: bfloat16 [8, 128, 128], P(None, 'mp'), may hold values from -0.5 to 0.5
- moment1: float32 [16, 128, 128], P('dp', 'mp'), may hold values from -6 to 6
- moment2: float32 [16, 128, 128], P('dp', 'mp'), may hold values from 0.25 to 4
- slot_of_block: int32 [8], replicated, may hold values from 0 to 15, as said below
- trainable: int32 [8], replicated, may hold values 0 or 1
- width_of_block: int32 [8], replicated, may hold values from 64 to 128
Outputs:
- moment1_new: float32 [16, 128, 128], P('dp', 'mp')
- moment2_new: float32 [16, 128, 128], P('dp', 'mp')
- weights_new: bfloat16 [8, 128, 128], P(None, 'mp')
- grad_rms: float32 [], replicated
The draws below stay inside these ranges and needn't reach their ends.
Inputs may be any that keep to these rules, and one draw needn't show every extreme that they name: `slot_of_block`: all values differ; slot s belongs to owner s // 2 of dp; every owner holds at most 2 blocks and some owner exactly 2.
All inputs are finite; a program needn't handle non-finite values.
Results may differ from the reference program's by a relative error of at most 0.001.
Values may be sent and summed in bfloat16 or wider, within the bound.
No kernel may reach another device: no remote copies, remote signals or barrier semaphores. Data moves between devices by JAX's collectives and lax.ppermute only.
A program may use at most 64 MiB of HBM per device.

```python
import math
import jax
import jax.numpy as jnp
from jax import lax

BS = 128
BLK_DEV = 1
STEP = 20
NB = 8
CAP = 2
SLOTS = 16


def draw_slot_of_block(key, part):
    first_key, second_key, third_key = jax.random.split(jax.random.fold_in(key, 17), 3)
    owners = jax.random.permutation(first_key, SLOTS // CAP)
    ordered = (owners[:, None] * CAP + jnp.arange(CAP, dtype=jnp.int32)[None, :]).reshape(-1)
    shuffled = jax.random.permutation(second_key, ordered[CAP:])
    chosen = jnp.concatenate([ordered[:CAP], shuffled])[:NB]
    return jax.random.permutation(third_key, chosen).astype(jnp.int32)


def draw_grads(key, part):
    base_key, pair_key = jax.random.split(jax.random.fold_in(key, 29), 2)
    replicas = NB // BLK_DEV
    pairing = jax.random.permutation(pair_key, NB)[:replicas]
    spike = 1.0 + 3.0 * (pairing[:, None] == jnp.arange(NB, dtype=jnp.int32)[None, :]).astype(jnp.float32)
    shape = (replicas, NB, BS, BS)
    base = jnp.clip(jax.random.normal(base_key, shape, jnp.float32), -6.0, 6.0)
    return (base * spike[:, :, None, None]).astype(jnp.bfloat16)


def place_ends(values, stream_key, smallest, largest):
    shape = values.shape
    place = [jax.random.randint(jax.random.fold_in(stream_key, axis), (), 0, shape[axis]) for axis in range(len(shape))]
    values = values.at[tuple(place)].set(smallest)
    longest = shape.index(max(shape))
    place[longest] = (place[longest] + 1) % shape[longest]
    return values.at[tuple(place)].set(largest)


def block_levels(stream_key, extent, cuts, low, high):
    loudness, own = 1.0, jax.random.fold_in(stream_key, 6)
    for axis_at, parts in cuts:
        heights = jnp.exp(jax.random.uniform(jax.random.fold_in(own, axis_at), (parts,), jnp.float32, low / len(cuts), high / len(cuts)))
        loudness = loudness * jnp.repeat(heights, extent[axis_at] // parts).reshape([-1 if axis == axis_at else 1 for axis in range(len(extent))])
    return loudness


def normal_values(key, dims, deviation, most, cuts=(), held_as=jnp.bfloat16):
    drawn = jax.random.normal(key, dims, jnp.float32) * deviation
    if len(cuts) > 0:
        drawn = block_levels(key, dims, cuts, -0.22, 0.18) * drawn
    return jnp.clip(drawn, min=-most, max=most).astype(held_as)


def setup_inputs(seed: int = 0) -> dict:
    arg_keys = jax.random.split(jax.random.key(seed), 8)
    return {
        "grads": draw_grads(jax.random.fold_in(arg_keys[7], 71), 0),
        "weights": normal_values(arg_keys[1], (NB, BS, BS), BS ** -0.5, 0.5, ((1, 4),)),
        "moment1": normal_values(arg_keys[2], (SLOTS, BS, BS), 1.0, 6.0, ((0, 8), (1, 4)), jnp.float32),
        "moment2": jnp.clip(jnp.exp(math.log(4.0) - 2.7725887 * jax.random.uniform(arg_keys[3], (SLOTS, BS, BS), jnp.float32) ** block_levels(arg_keys[3], (SLOTS, BS, BS), ((0, 8), (1, 4)), -0.2, 0.2)), 0.25, 4.0),
        "slot_of_block": draw_slot_of_block(jax.random.fold_in(arg_keys[7], 71), 0),
        "trainable": place_ends((jax.random.randint(arg_keys[5], (NB,), 0, 2) < 1).astype(jnp.int32), jax.random.fold_in(arg_keys[5], 1), 0, 1),
        "width_of_block": place_ends(jax.random.randint(arg_keys[6], (NB,), BS // 2, BS + 1), jax.random.fold_in(arg_keys[6], 1), BS // 2, BS).astype(jnp.int32),
    }


def reference(grads, weights, moment1, moment2, slot_of_block, trainable, width_of_block):
    total = lax.optimization_barrier(jnp.sum(grads.astype(jnp.float32), axis=0))
    columns = jnp.arange(BS, dtype=jnp.int32)
    live = ((trainable[:, None] > 0) & (columns[None, :] < width_of_block[:, None])).astype(jnp.float32)
    sumsq = jnp.sum(total * total * live[:, None, :])
    count = jnp.sum(live) * BS
    grad_rms = jnp.sqrt(sumsq) / jnp.sqrt(jnp.maximum(count, 1.0))
    clip = 1.0 / jnp.maximum(grad_rms, 1.0)
    block_ids = jnp.arange(NB, dtype=jnp.int32)
    occupied = jnp.zeros((SLOTS,), jnp.int32).at[slot_of_block].set(1)
    block_of_slot = jnp.zeros((SLOTS,), jnp.int32).at[slot_of_block].set(block_ids)
    slot_grad = total[block_of_slot] * occupied[:, None, None].astype(jnp.float32)
    slot_live = live[block_of_slot] * occupied[:, None].astype(jnp.float32)
    update_mask = slot_live[:, None, :] > 0
    clipped = clip * slot_grad
    first_new = jnp.where(update_mask, 0.9 * moment1 + 0.1 * clipped, moment1)
    second_new = jnp.where(update_mask, 0.95 * moment2 + 0.05 * clipped * clipped, moment2)
    direction = first_new / (1.0 - 0.9 ** STEP) / (jnp.sqrt(second_new / (1.0 - 0.95 ** STEP)) + 1e-08)
    slot_weight = weights[block_of_slot].astype(jnp.float32)
    slot_new = jnp.where(update_mask, slot_weight - 0.001 * (direction + 0.1 * slot_weight), slot_weight)
    weights_new = slot_new.astype(jnp.bfloat16)[slot_of_block]
    return (first_new, second_new, weights_new, grad_rms)
```

```python
import functools

import jax
import jax.numpy as jnp
from jax import lax
from jax.experimental import pallas as pl
from jax.experimental.pallas import tpu as pltpu
from jax.sharding import PartitionSpec as P

STEP = 20
GATHER_BYTES = 4 << 20


F32 = jnp.float32


def tree_sum(terms):
    while len(terms) > 1:
        terms = [terms[i] + terms[i + 1] for i in range(0, len(terms), 2)]
    return terms[0]


def xor_pairs(size, k):
    return [(j, j ^ k) for j in range(size)]


def live_width(trainable_ref, width_ref, b, block_size):
    width = jnp.clip(width_ref[b], 0, block_size)
    return jnp.where(trainable_ref[b] > 0, width, 0)


def total_kernel(replicas, trainable_ref, width_ref, *refs):
    grad_refs, total_ref, part_ref = refs[:replicas], refs[replicas], refs[replicas + 1]
    blocks, rows, cols = total_ref.shape
    column = lax.broadcasted_iota(jnp.int32, (rows, cols), 1)
    squares = jnp.zeros((rows, cols), F32)
    for b in range(blocks):
        total = tree_sum([ref[b].astype(F32) for ref in grad_refs])
        total_ref[b] = total
        width = live_width(trainable_ref, width_ref, b, cols)
        squares = squares + jnp.where(column < width, total * total, 0.0)
    part_ref[...] = jnp.full(part_ref.shape, jnp.sum(squares), F32)


def step_kernel(
    parts,
    owner_ref,
    slot_ref,
    trainable_ref,
    width_ref,
    *refs,
):
    part_refs = refs[:parts]
    total_ref, weight_ref, first_ref, second_ref, moments_ref = refs[parts : parts + 5]
    first_out, second_out, weight_out, rms_out = refs[parts + 5 :]
    blocks, rows, cols = total_ref.shape
    capacity = first_ref.shape[0]
    owner = owner_ref[0]
    column = lax.broadcasted_iota(jnp.int32, (rows, cols), 1)

    sumsq = tree_sum([ref[...] for ref in part_refs])[0:1]
    widths = [live_width(trainable_ref, width_ref, b, cols) for b in range(blocks)]
    count = functools.reduce(lambda x, y: x + y, widths).astype(F32) * float(cols)
    count = jnp.full(sumsq.shape, jnp.maximum(count, 1.0), F32)
    grad_rms = jnp.sqrt(sumsq) / jnp.sqrt(count)
    rms_out[0] = jnp.max(grad_rms)
    clip = 1.0 / jnp.maximum(grad_rms, 1.0)

    def moments_of(total, first, second):
        clipped = clip * total
        return 0.9 * first + 0.1 * clipped, 0.95 * second + 0.05 * clipped * clipped

    for c in range(capacity):
        block, width = jnp.int32(0), jnp.int32(0)
        for b in range(blocks):
            here = slot_ref[b] == owner * capacity + c
            block = jnp.where(here, b, block)
            width = jnp.where(here, widths[b], width)
        first, second = first_ref[c], second_ref[c]
        first_new, second_new = moments_of(total_ref[block], first, second)
        first_out[c] = jnp.where(column < width, first_new, first)
        second_out[c] = jnp.where(column < width, second_new, second)

    for b in range(blocks):
        slot = slot_ref[b]
        near = (slot // capacity) ^ owner
        held = slot % capacity
        first_new, second_new = moments_of(
            total_ref[b], moments_ref[near, 0, held], moments_ref[near, 1, held]
        )
        direction = (
            first_new
            / (1.0 - 0.9**STEP)
            / (jnp.sqrt(second_new / (1.0 - 0.95**STEP)) + 1e-08)
        )
        weight = weight_ref[b].astype(F32)
        weight_new = weight - 0.001 * (direction + 0.1 * weight)
        weight_out[b] = jnp.where(column < widths[b], weight_new, weight).astype(
            weight_out.dtype
        )


def gathered(
    replicas,
    shares,
    grads,
    weights,
    moment1,
    moment2,
    slot_of_block,
    trainable,
    width_of_block,
):
    own = grads[0]
    blocks, rows, cols = own.shape
    capacity = moment1.shape[0]
    owner = lax.axis_index("dp").astype(jnp.int32).reshape(1)
    smem = pl.BlockSpec(memory_space=pltpu.SMEM)
    vmem = pl.BlockSpec(memory_space=pltpu.VMEM)

    moments = jnp.stack([moment1, moment2]).astype(jnp.float16)
    grad_terms = [own] + [
        lax.ppermute(own, "dp", xor_pairs(replicas, k)) for k in range(1, replicas)
    ]
    pair = jnp.stack([moments, lax.ppermute(moments, "dp", xor_pairs(replicas, 1))])
    all_moments = jnp.concatenate(
        [pair]
        + [lax.ppermute(pair, "dp", xor_pairs(replicas, k)) for k in range(2, replicas, 2)]
    ).astype(F32)

    total, part = pl.pallas_call(
        functools.partial(total_kernel, replicas),
        out_shape=(
            jax.ShapeDtypeStruct((blocks, rows, cols), F32),
            jax.ShapeDtypeStruct((8, cols), F32),
        ),
        in_specs=[smem] * 2 + [vmem] * replicas,
        out_specs=(vmem, vmem),
    )(trainable, width_of_block, *grad_terms)
    parts = [part] + [
        lax.ppermute(part, "mp", xor_pairs(shares, k)) for k in range(1, shares)
    ]
    first_new, second_new, weights_new, grad_rms = pl.pallas_call(
        functools.partial(step_kernel, shares),
        out_shape=(
            jax.ShapeDtypeStruct(moment1.shape, F32),
            jax.ShapeDtypeStruct(moment2.shape, F32),
            jax.ShapeDtypeStruct(weights.shape, weights.dtype),
            jax.ShapeDtypeStruct((1,), F32),
        ),
        in_specs=[smem] * 4 + [vmem] * (shares + 5),
        out_specs=(vmem, vmem, vmem, smem),
    )(
        owner,
        slot_of_block,
        trainable,
        width_of_block,
        *parts,
        total,
        weights,
        moment1,
        moment2,
        all_moments,
    )
    return first_new, second_new, weights_new, grad_rms.reshape(())


def reduced(grads, weights, moment1, moment2, slot_of_block, trainable, width_of_block):
    blocks, row_share, block_size = weights.shape
    capacity = moment1.shape[0]
    local_grads = grads[0].reshape(blocks, row_share * block_size)
    own_slots = lax.axis_index("dp") * capacity + jnp.arange(capacity, dtype=jnp.int32)
    owned_onehot = slot_of_block[None, :] == own_slots[:, None]
    columns = jnp.arange(block_size, dtype=jnp.int32)
    live = (
        (trainable[:, None] > 0) & (columns[None, :] < width_of_block[:, None])
    ).astype(F32)
    slot_live = jnp.dot(owned_onehot.astype(F32), live, precision=lax.Precision.HIGHEST)
    count = jnp.sum(live) * block_size
    summed = lax.psum(local_grads.astype(F32), "dp")
    summed_blocks = summed.reshape(blocks, row_share, block_size)
    sumsq = lax.psum(jnp.sum(summed_blocks * summed_blocks * live[:, None, :]), "mp")
    slot_grad = jnp.dot(
        owned_onehot.astype(F32), summed, precision=lax.Precision.HIGHEST
    ).reshape(capacity, row_share, block_size)
    grad_rms = jnp.sqrt(sumsq) / jnp.sqrt(jnp.maximum(count, 1.0))
    clip = 1.0 / jnp.maximum(grad_rms, 1.0)
    update_mask = slot_live[:, None, :] > 0
    clipped = clip * slot_grad
    first_new = jnp.where(update_mask, 0.9 * moment1 + 0.1 * clipped, moment1)
    second_new = jnp.where(
        update_mask, 0.95 * moment2 + 0.05 * clipped * clipped, moment2
    )
    direction = (
        first_new
        / (1.0 - 0.9**STEP)
        / (jnp.sqrt(second_new / (1.0 - 0.95**STEP)) + 1e-08)
    )
    slot_weight = jnp.dot(
        owned_onehot.astype(jnp.bfloat16),
        weights.reshape(blocks, row_share * block_size),
        preferred_element_type=F32,
    ).reshape(capacity, row_share, block_size)
    slot_new = jnp.where(
        update_mask, slot_weight - 0.001 * (direction + 0.1 * slot_weight), slot_weight
    )
    slot_new = slot_new.astype(jnp.bfloat16).reshape(capacity, row_share * block_size)
    every_slot = lax.all_gather(slot_new, "dp", axis=0, tiled=True)
    slots = jnp.arange(every_slot.shape[0], dtype=jnp.int32)
    placing = (slot_of_block[:, None] == slots[None, :]).astype(jnp.bfloat16)
    weights_new = jnp.dot(placing, every_slot, preferred_element_type=F32).astype(
        jnp.bfloat16
    )
    return (
        first_new,
        second_new,
        weights_new.reshape(blocks, row_share, block_size),
        grad_rms,
    )


def local(replicas, shares, grads, *rest):
    two_powers = replicas & (replicas - 1) == 0 and shares & (shares - 1) == 0
    if two_powers and replicas > 1 and replicas * grads.nbytes <= GATHER_BYTES:
        return gathered(replicas, shares, grads, *rest)
    return reduced(grads, *rest)


def solution(mesh):
    return jax.shard_map(
        functools.partial(local, mesh.shape["dp"], mesh.shape["mp"]),
        mesh=mesh,
        in_specs=(
            P("dp", None, "mp", None),
            P(None, "mp", None),
            P("dp", "mp", None),
            P("dp", "mp", None),
            P(),
            P(),
            P(),
        ),
        out_specs=(P("dp", "mp", None), P("dp", "mp", None), P(None, "mp", None), P()),
        check_vma=False,
    )
```

```python
import functools

import jax
import jax.numpy as jnp
from jax import lax
from jax.experimental import pallas as pl
from jax.experimental.pallas import tpu as pltpu
from jax.sharding import PartitionSpec as P


STEP = 20
GATHER_BYTES = 4 << 20


F32 = jnp.float32
VMEM_BYTES = 8 << 20
STAGES = [[4], [2], [1]]


def tree_sum(terms):
    while len(terms) > 1:
        terms = [terms[i] + terms[i + 1] for i in range(0, len(terms), 2)]
    return terms[0]


def xor_pairs(size, k):
    return [(j, j ^ k) for j in range(size)]


def live_width(trainable_ref, width_ref, b, block_size):
    width = jnp.clip(width_ref[b], 0, block_size)
    return jnp.where(trainable_ref[b] > 0, width, 0)


def shape_of(*dims, dtype=F32):
    return jax.ShapeDtypeStruct(dims, dtype)


def kernel_call(body, out_shape, scalars, *operands, out_smem=()):
    smem = pl.BlockSpec(memory_space=pltpu.SMEM)
    vmem = pl.BlockSpec(memory_space=pltpu.VMEM)
    return pl.pallas_call(
        body,
        out_shape=out_shape,
        in_specs=[smem] * len(scalars) + [vmem] * len(operands),
        out_specs=tuple(smem if i in out_smem else vmem for i in range(len(out_shape))),
        compiler_params=pltpu.CompilerParams(vmem_limit_bytes=VMEM_BYTES),
    )(*scalars, *operands)


def mask_kernel(trainable_ref, width_ref, weight_ref, live_ref, norm_ref, wide_ref):
    blocks, rows, cols = live_ref.shape
    column = lax.broadcasted_iota(jnp.int32, (rows, cols), 1)
    count = jnp.int32(0)
    for b in range(blocks):
        width = live_width(trainable_ref, width_ref, b, cols)
        count = count + width
        live_ref[b] = (column < width).astype(F32)
        wide_ref[b] = weight_ref[b].astype(F32)
    count = count.astype(F32) * float(cols)
    norm_ref[...] = jnp.sqrt(jnp.full(norm_ref.shape, jnp.maximum(count, 1.0), F32))


def total_kernel(terms, live_ref, *refs):
    grad_refs, total_ref, part_ref = refs[:terms], refs[terms], refs[terms + 1]
    blocks, rows, cols = total_ref.shape
    squares = jnp.zeros((rows, cols), F32)
    for b in range(blocks):
        total = tree_sum([ref[b].astype(F32) for ref in grad_refs])
        total_ref[b] = total
        squares = squares + live_ref[b] * (total * total)
    part_ref[...] = jnp.full(part_ref.shape, jnp.sum(squares), F32)


def placing_kernel(
    order,
    owner_ref,
    slot_ref,
    total_ref,
    live_ref,
    moments_ref,
    block_first_ref,
    block_second_ref,
    slot_total_ref,
    slot_live_ref,
):
    blocks = total_ref.shape[0]
    capacity = slot_total_ref.shape[0]
    owner = owner_ref[0]
    for b in range(blocks):
        slot = slot_ref[b]
        near = (slot // capacity) ^ owner
        near = sum(jnp.where(near == k, order[k], 0) for k in range(len(order)))
        held = slot % capacity
        block_first_ref[b] = moments_ref[near, 0, held]
        block_second_ref[b] = moments_ref[near, 1, held]
    for c in range(capacity):
        block, used = jnp.int32(0), jnp.int32(0)
        for b in range(blocks):
            here = slot_ref[b] == owner * capacity + c
            block = jnp.where(here, b, block)
            used = jnp.where(here, 1, used)
        slot_total_ref[c] = total_ref[block]
        slot_live_ref[c] = live_ref[block] * used.astype(F32)


def step_kernel(parts, *refs):
    part_refs = refs[:parts]
    (
        total_ref,
        live_ref,
        norm_ref,
        wide_ref,
        block_first_ref,
        block_second_ref,
        slot_total_ref,
        slot_live_ref,
        first_ref,
        second_ref,
    ) = refs[parts : parts + 10]
    first_out, second_out, weight_out, rms_out = refs[parts + 10 :]
    blocks = total_ref.shape[0]
    capacity = first_ref.shape[0]

    sumsq = tree_sum([ref[...] for ref in part_refs])
    grad_rms = jnp.sqrt(sumsq) / norm_ref[...]
    clip = (1.0 / jnp.maximum(grad_rms, 1.0))[0:1]

    def moments_of(total, first, second):
        clipped = clip * total
        return 0.9 * first + 0.1 * clipped, 0.95 * second + 0.05 * clipped * clipped

    for b in range(blocks):
        first_new, second_new = moments_of(
            total_ref[b], block_first_ref[b], block_second_ref[b]
        )
        direction = (
            first_new
            / (1.0 - 0.9**STEP)
            / (jnp.sqrt(second_new / (1.0 - 0.95**STEP)) + 1e-08)
        )
        weight = wide_ref[b]
        weight_new = weight - 0.001 * (direction + 0.1 * weight)
        weight_out[b] = jnp.where(live_ref[b] > 0, weight_new, weight).astype(
            weight_out.dtype
        )
    for c in range(capacity):
        first, second = first_ref[c], second_ref[c]
        first_new, second_new = moments_of(slot_total_ref[c], first, second)
        first_out[c] = jnp.where(slot_live_ref[c] > 0, first_new, first)
        second_out[c] = jnp.where(slot_live_ref[c] > 0, second_new, second)
    rms_out[0] = jnp.max(grad_rms)


def gathered(
    replicas,
    shares,
    grads,
    weights,
    moment1,
    moment2,
    slot_of_block,
    trainable,
    width_of_block,
):
    own = grads[0]
    blocks, rows, cols = own.shape
    owner = lax.axis_index("dp").astype(jnp.int32).reshape(1)
    full = (blocks, rows, cols)
    tile = (8, cols)

    def send(x, axis, size, k):
        return lax.ppermute(x, axis, xor_pairs(size, k))

    moments = jnp.stack([moment1, moment2]).astype(jnp.float16)[None]
    offsets = [0]
    carried = own
    for stage, ks in enumerate(STAGES):
        terms = [carried] + [send(carried, "dp", replicas, k) for k in ks]
        moments = jnp.concatenate(
            [moments] + [send(moments, "dp", replicas, k) for k in ks]
        )
        offsets = [k ^ o for k in [0] + ks for o in offsets]
        if stage < len(STAGES) - 1:
            carried = tree_sum([t.astype(F32) for t in terms])
    order = [offsets.index(k) for k in range(replicas)]

    live, norm, wide = kernel_call(
        mask_kernel,
        (shape_of(*full), shape_of(*tile), shape_of(*full)),
        (trainable, width_of_block),
        weights,
    )
    total, part = kernel_call(
        functools.partial(total_kernel, len(terms)),
        (shape_of(*full), shape_of(*tile)),
        (),
        live,
        *terms,
    )
    parts = [part] + [send(part, "mp", shares, k) for k in range(1, shares)]
    placed = kernel_call(
        functools.partial(placing_kernel, order),
        (
            shape_of(*full),
            shape_of(*full),
            shape_of(*moment1.shape),
            shape_of(*moment1.shape),
        ),
        (owner, slot_of_block),
        total,
        live,
        moments.astype(F32),
    )
    first_new, second_new, weights_new, grad_rms = kernel_call(
        functools.partial(step_kernel, shares),
        (
            shape_of(*moment1.shape),
            shape_of(*moment2.shape),
            shape_of(*full, dtype=weights.dtype),
            shape_of(1),
        ),
        (),
        *parts,
        total,
        live,
        norm,
        wide,
        *placed,
        moment1,
        moment2,
        out_smem=(3,),
    )
    return first_new, second_new, weights_new, grad_rms.reshape(())


def reduced(grads, weights, moment1, moment2, slot_of_block, trainable, width_of_block):
    blocks, row_share, block_size = weights.shape
    capacity = moment1.shape[0]
    local_grads = grads[0].reshape(blocks, row_share * block_size)
    own_slots = lax.axis_index("dp") * capacity + jnp.arange(capacity, dtype=jnp.int32)
    owned_onehot = slot_of_block[None, :] == own_slots[:, None]
    columns = jnp.arange(block_size, dtype=jnp.int32)
    live = (
        (trainable[:, None] > 0) & (columns[None, :] < width_of_block[:, None])
    ).astype(F32)
    slot_live = jnp.dot(owned_onehot.astype(F32), live, precision=lax.Precision.HIGHEST)
    count = jnp.sum(live) * block_size
    summed = lax.psum(local_grads.astype(F32), "dp")
    summed_blocks = summed.reshape(blocks, row_share, block_size)
    sumsq = lax.psum(jnp.sum(summed_blocks * summed_blocks * live[:, None, :]), "mp")
    slot_grad = jnp.dot(
        owned_onehot.astype(F32), summed, precision=lax.Precision.HIGHEST
    ).reshape(capacity, row_share, block_size)
    grad_rms = jnp.sqrt(sumsq) / jnp.sqrt(jnp.maximum(count, 1.0))
    clip = 1.0 / jnp.maximum(grad_rms, 1.0)
    update_mask = slot_live[:, None, :] > 0
    clipped = clip * slot_grad
    first_new = jnp.where(update_mask, 0.9 * moment1 + 0.1 * clipped, moment1)
    second_new = jnp.where(
        update_mask, 0.95 * moment2 + 0.05 * clipped * clipped, moment2
    )
    direction = (
        first_new
        / (1.0 - 0.9**STEP)
        / (jnp.sqrt(second_new / (1.0 - 0.95**STEP)) + 1e-08)
    )
    slot_weight = jnp.dot(
        owned_onehot.astype(jnp.bfloat16),
        weights.reshape(blocks, row_share * block_size),
        preferred_element_type=F32,
    ).reshape(capacity, row_share, block_size)
    slot_new = jnp.where(
        update_mask, slot_weight - 0.001 * (direction + 0.1 * slot_weight), slot_weight
    )
    slot_new = slot_new.astype(jnp.bfloat16).reshape(capacity, row_share * block_size)
    every_slot = lax.all_gather(slot_new, "dp", axis=0, tiled=True)
    slots = jnp.arange(every_slot.shape[0], dtype=jnp.int32)
    placing = (slot_of_block[:, None] == slots[None, :]).astype(jnp.bfloat16)
    weights_new = jnp.dot(placing, every_slot, preferred_element_type=F32).astype(
        jnp.bfloat16
    )
    return (
        first_new,
        second_new,
        weights_new.reshape(blocks, row_share, block_size),
        grad_rms,
    )


def local(replicas, shares, grads, *rest):
    two_powers = replicas & (replicas - 1) == 0 and shares & (shares - 1) == 0
    if two_powers and replicas > 1 and replicas * grads.nbytes <= GATHER_BYTES:
        return gathered(replicas, shares, grads, *rest)
    return reduced(grads, *rest)


def solution(mesh):
    return jax.shard_map(
        functools.partial(local, mesh.shape["dp"], mesh.shape["mp"]),
        mesh=mesh,
        in_specs=(
            P("dp", None, "mp", None),
            P(None, "mp", None),
            P("dp", "mp", None),
            P("dp", "mp", None),
            P(),
            P(),
            P(),
        ),
        out_specs=(P("dp", "mp", None), P("dp", "mp", None), P(None, "mp", None), P()),
        check_vma=False,
    )
```

```python
import functools

import jax
import jax.numpy as jnp
from jax import lax
from jax.experimental import pallas as pl
from jax.experimental.pallas import tpu as pltpu
from jax.sharding import PartitionSpec as P


STEP = 20
GATHER_BYTES = 4 << 20


F32 = jnp.float32
VMEM_BYTES = 8 << 20
STAGES = [[4, 4], [2, 1], [1, 2]]


def tree_sum(terms):
    while len(terms) > 1:
        terms = [terms[i] + terms[i + 1] for i in range(0, len(terms), 2)]
    return terms[0]


def xor_pairs(size, k):
    return [(j, j ^ k) for j in range(size)]


def staged_pairs(replicas, shares, ks):
    pairs = []
    for j in range(replicas):
        for m in range(shares):
            pairs.append((j * shares + m, (j ^ ks[m % len(ks)]) * shares + m))
    return pairs


def live_width(trainable_ref, width_ref, b, block_size):
    width = jnp.clip(width_ref[b], 0, block_size)
    return jnp.where(trainable_ref[b] > 0, width, 0)


def shape_of(*dims, dtype=F32):
    return jax.ShapeDtypeStruct(dims, dtype)


def kernel_call(body, out_shape, scalars, *operands, out_smem=()):
    smem = pl.BlockSpec(memory_space=pltpu.SMEM)
    vmem = pl.BlockSpec(memory_space=pltpu.VMEM)
    return pl.pallas_call(
        body,
        out_shape=out_shape,
        in_specs=[smem] * len(scalars) + [vmem] * len(operands),
        out_specs=tuple(smem if i in out_smem else vmem for i in range(len(out_shape))),
        compiler_params=pltpu.CompilerParams(vmem_limit_bytes=VMEM_BYTES),
    )(*scalars, *operands)


def mask_kernel(trainable_ref, width_ref, weight_ref, live_ref, norm_ref, wide_ref):
    blocks, rows, cols = live_ref.shape
    column = lax.broadcasted_iota(jnp.int32, (rows, cols), 1)
    count = jnp.int32(0)
    for b in range(blocks):
        width = live_width(trainable_ref, width_ref, b, cols)
        count = count + width
        live_ref[b] = (column < width).astype(F32)
        wide_ref[b] = weight_ref[b].astype(F32)
    count = count.astype(F32) * float(cols)
    norm_ref[...] = jnp.sqrt(jnp.full(norm_ref.shape, jnp.maximum(count, 1.0), F32))


def total_kernel(terms, live_ref, *refs):
    grad_refs, total_ref, part_ref = refs[:terms], refs[terms], refs[terms + 1]
    blocks, rows, cols = total_ref.shape
    squares = jnp.zeros((rows, cols), F32)
    for b in range(blocks):
        total = tree_sum([ref[b].astype(F32) for ref in grad_refs])
        total_ref[b] = total
        squares = squares + live_ref[b] * (total * total)
    part_ref[...] = jnp.full(part_ref.shape, jnp.sum(squares), F32)


def placing_kernel(
    order,
    owner_ref,
    slot_ref,
    total_ref,
    live_ref,
    moments_ref,
    block_first_ref,
    block_second_ref,
    slot_total_ref,
    slot_live_ref,
):
    blocks = total_ref.shape[0]
    capacity = slot_total_ref.shape[0]
    owner = owner_ref[0]
    for b in range(blocks):
        slot = slot_ref[b]
        near = (slot // capacity) ^ owner
        near = sum(
            jnp.where(near == k, jnp.where(owner_ref[1] == 0, order[0][k], order[1][k]), 0)
            for k in range(len(order[0]))
        )
        held = slot % capacity
        block_first_ref[b] = moments_ref[near, 0, held]
        block_second_ref[b] = moments_ref[near, 1, held]
    for c in range(capacity):
        block, used = jnp.int32(0), jnp.int32(0)
        for b in range(blocks):
            here = slot_ref[b] == owner * capacity + c
            block = jnp.where(here, b, block)
            used = jnp.where(here, 1, used)
        slot_total_ref[c] = total_ref[block]
        slot_live_ref[c] = live_ref[block] * used.astype(F32)


def step_kernel(parts, *refs):
    part_refs = refs[:parts]
    (
        total_ref,
        live_ref,
        norm_ref,
        wide_ref,
        block_first_ref,
        block_second_ref,
        slot_total_ref,
        slot_live_ref,
        first_ref,
        second_ref,
    ) = refs[parts : parts + 10]
    first_out, second_out, weight_out, rms_out = refs[parts + 10 :]
    blocks = total_ref.shape[0]
    capacity = first_ref.shape[0]

    sumsq = tree_sum([ref[...] for ref in part_refs])
    grad_rms = jnp.sqrt(sumsq) / norm_ref[...]
    clip = (1.0 / jnp.maximum(grad_rms, 1.0))[0:1]

    def moments_of(total, first, second):
        clipped = clip * total
        return 0.9 * first + 0.1 * clipped, 0.95 * second + 0.05 * clipped * clipped

    for b in range(blocks):
        first_new, second_new = moments_of(
            total_ref[b], block_first_ref[b], block_second_ref[b]
        )
        direction = (
            first_new
            / (1.0 - 0.9**STEP)
            / (jnp.sqrt(second_new / (1.0 - 0.95**STEP)) + 1e-08)
        )
        weight = wide_ref[b]
        weight_new = weight - 0.001 * (direction + 0.1 * weight)
        weight_out[b] = jnp.where(live_ref[b] > 0, weight_new, weight).astype(
            weight_out.dtype
        )
    for c in range(capacity):
        first, second = first_ref[c], second_ref[c]
        first_new, second_new = moments_of(slot_total_ref[c], first, second)
        first_out[c] = jnp.where(slot_live_ref[c] > 0, first_new, first)
        second_out[c] = jnp.where(slot_live_ref[c] > 0, second_new, second)
    rms_out[0] = jnp.max(grad_rms)


def gathered(
    replicas,
    shares,
    grads,
    weights,
    moment1,
    moment2,
    slot_of_block,
    trainable,
    width_of_block,
):
    own = grads[0]
    blocks, rows, cols = own.shape
    owner = jnp.stack([lax.axis_index("dp"), lax.axis_index("mp") % 2]).astype(jnp.int32)
    full = (blocks, rows, cols)
    tile = (8, cols)

    def send(x, axis, size, k):
        return lax.ppermute(x, axis, xor_pairs(size, k))

    def exchange(x, ks):
        return lax.ppermute(x, ("dp", "mp"), staged_pairs(replicas, shares, ks))

    moments = jnp.stack([moment1, moment2]).astype(jnp.float16)[None]
    offsets = [[0], [0]]
    carried = own
    for stage, ks in enumerate(STAGES):
        terms = [carried, exchange(carried, ks)]
        moments = jnp.concatenate([moments, exchange(moments, ks)])
        offsets = [[k ^ o for k in (0, ks[i]) for o in offsets[i]] for i in range(2)]
        if stage < len(STAGES) - 1:
            carried = tree_sum([t.astype(F32) for t in terms])
    order = [[of.index(k) for k in range(replicas)] for of in offsets]

    live, norm, wide = kernel_call(
        mask_kernel,
        (shape_of(*full), shape_of(*tile), shape_of(*full)),
        (trainable, width_of_block),
        weights,
    )
    total, part = kernel_call(
        functools.partial(total_kernel, len(terms)),
        (shape_of(*full), shape_of(*tile)),
        (),
        live,
        *terms,
    )
    parts = [part] + [send(part, "mp", shares, k) for k in range(1, shares)]
    placed = kernel_call(
        functools.partial(placing_kernel, order),
        (
            shape_of(*full),
            shape_of(*full),
            shape_of(*moment1.shape),
            shape_of(*moment1.shape),
        ),
        (owner, slot_of_block),
        total,
        live,
        moments.astype(F32),
    )
    first_new, second_new, weights_new, grad_rms = kernel_call(
        functools.partial(step_kernel, shares),
        (
            shape_of(*moment1.shape),
            shape_of(*moment2.shape),
            shape_of(*full, dtype=weights.dtype),
            shape_of(1),
        ),
        (),
        *parts,
        total,
        live,
        norm,
        wide,
        *placed,
        moment1,
        moment2,
        out_smem=(3,),
    )
    return first_new, second_new, weights_new, grad_rms.reshape(())


def reduced(grads, weights, moment1, moment2, slot_of_block, trainable, width_of_block):
    blocks, row_share, block_size = weights.shape
    capacity = moment1.shape[0]
    local_grads = grads[0].reshape(blocks, row_share * block_size)
    own_slots = lax.axis_index("dp") * capacity + jnp.arange(capacity, dtype=jnp.int32)
    owned_onehot = slot_of_block[None, :] == own_slots[:, None]
    columns = jnp.arange(block_size, dtype=jnp.int32)
    live = (
        (trainable[:, None] > 0) & (columns[None, :] < width_of_block[:, None])
    ).astype(F32)
    slot_live = jnp.dot(owned_onehot.astype(F32), live, precision=lax.Precision.HIGHEST)
    count = jnp.sum(live) * block_size
    summed = lax.psum(local_grads.astype(F32), "dp")
    summed_blocks = summed.reshape(blocks, row_share, block_size)
    sumsq = lax.psum(jnp.sum(summed_blocks * summed_blocks * live[:, None, :]), "mp")
    slot_grad = jnp.dot(
        owned_onehot.astype(F32), summed, precision=lax.Precision.HIGHEST
    ).reshape(capacity, row_share, block_size)
    grad_rms = jnp.sqrt(sumsq) / jnp.sqrt(jnp.maximum(count, 1.0))
    clip = 1.0 / jnp.maximum(grad_rms, 1.0)
    update_mask = slot_live[:, None, :] > 0
    clipped = clip * slot_grad
    first_new = jnp.where(update_mask, 0.9 * moment1 + 0.1 * clipped, moment1)
    second_new = jnp.where(
        update_mask, 0.95 * moment2 + 0.05 * clipped * clipped, moment2
    )
    direction = (
        first_new
        / (1.0 - 0.9**STEP)
        / (jnp.sqrt(second_new / (1.0 - 0.95**STEP)) + 1e-08)
    )
    slot_weight = jnp.dot(
        owned_onehot.astype(jnp.bfloat16),
        weights.reshape(blocks, row_share * block_size),
        preferred_element_type=F32,
    ).reshape(capacity, row_share, block_size)
    slot_new = jnp.where(
        update_mask, slot_weight - 0.001 * (direction + 0.1 * slot_weight), slot_weight
    )
    slot_new = slot_new.astype(jnp.bfloat16).reshape(capacity, row_share * block_size)
    every_slot = lax.all_gather(slot_new, "dp", axis=0, tiled=True)
    slots = jnp.arange(every_slot.shape[0], dtype=jnp.int32)
    placing = (slot_of_block[:, None] == slots[None, :]).astype(jnp.bfloat16)
    weights_new = jnp.dot(placing, every_slot, preferred_element_type=F32).astype(
        jnp.bfloat16
    )
    return (
        first_new,
        second_new,
        weights_new.reshape(blocks, row_share, block_size),
        grad_rms,
    )


def local(replicas, shares, grads, *rest):
    two_powers = replicas & (replicas - 1) == 0 and shares & (shares - 1) == 0
    if two_powers and replicas > 1 and replicas * grads.nbytes <= GATHER_BYTES:
        return gathered(replicas, shares, grads, *rest)
    return reduced(grads, *rest)


def solution(mesh):
    return jax.shard_map(
        functools.partial(local, mesh.shape["dp"], mesh.shape["mp"]),
        mesh=mesh,
        in_specs=(
            P("dp", None, "mp", None),
            P(None, "mp", None),
            P("dp", "mp", None),
            P("dp", "mp", None),
            P(),
            P(),
            P(),
        ),
        out_specs=(P("dp", "mp", None), P("dp", "mp", None), P(None, "mp", None), P()),
        check_vma=False,
    )
```

```python
import functools

import jax
import jax.numpy as jnp
from jax import lax
from jax.experimental import pallas as pl
from jax.experimental.pallas import tpu as pltpu
from jax.sharding import PartitionSpec as P


STEP = 20
RATE, DECAY = 0.001, 0.1
GATHER_BYTES = 4 << 20


F32 = jnp.float32
VMEM_BYTES = 8 << 20
STAGES = [[4, 1], [2, 2], [1, 4]]
MSTAGES = [[4, 1], [2, 2], [1, 4]]


def tree_sum(terms):
    while len(terms) > 1:
        terms = [terms[i] + terms[i + 1] for i in range(0, len(terms), 2)]
    return terms[0]


def xor_pairs(size, k):
    return [(j, j ^ k) for j in range(size)]


def staged_pairs(replicas, shares, ks):
    pairs = []
    for j in range(replicas):
        for m in range(shares):
            pairs.append((j * shares + m, (j ^ ks[m % len(ks)]) * shares + m))
    return pairs


def live_width(trainable_ref, width_ref, b, block_size):
    width = jnp.clip(width_ref[b], 0, block_size)
    return jnp.where(trainable_ref[b] > 0, width, 0)


def shape_of(*dims, dtype=F32):
    return jax.ShapeDtypeStruct(dims, dtype)


def kernel_call(body, out_shape, scalars, *operands, out_smem=()):
    smem = pl.BlockSpec(memory_space=pltpu.SMEM)
    vmem = pl.BlockSpec(memory_space=pltpu.VMEM)
    return pl.pallas_call(
        body,
        out_shape=out_shape,
        in_specs=[smem] * len(scalars) + [vmem] * len(operands),
        out_specs=tuple(smem if i in out_smem else vmem for i in range(len(out_shape))),
        compiler_params=pltpu.CompilerParams(vmem_limit_bytes=VMEM_BYTES),
    )(*scalars, *operands)


def mask_kernel(owner_ref, slot_ref, trainable_ref, width_ref, weight_ref, live_ref, norm_ref, wide_ref):
    blocks, rows, cols = live_ref.shape
    column = lax.broadcasted_iota(jnp.int32, (rows, cols), 1)
    count = jnp.int32(0)
    for b in range(blocks):
        width = live_width(trainable_ref, width_ref, b, cols)
        count = count + width
        live_ref[b] = (column < width).astype(F32)
        weight = weight_ref[b].astype(F32)
        wide_ref[b] = jnp.where(column < width, weight * (1.0 - RATE * DECAY), weight)
    count = count.astype(F32) * float(cols)
    norm_ref[...] = jnp.sqrt(jnp.full(norm_ref.shape, jnp.maximum(count, 1.0), F32))


def total_kernel(terms, live_ref, *refs):
    grad_refs, total_ref, part_ref = refs[:terms], refs[terms], refs[terms + 1]
    blocks, rows, cols = total_ref.shape
    squares = jnp.zeros((rows, cols), F32)
    for b in range(blocks):
        total = tree_sum([ref[b].astype(F32) for ref in grad_refs])
        total_ref[b] = total
        squares = squares + live_ref[b] * (total * total)
    part_ref[...] = jnp.full(part_ref.shape, jnp.sum(squares), F32)


def placing_kernel(
    order,
    owner_ref,
    slot_ref,
    total_ref,
    live_ref,
    moments_ref,
    block_first_ref,
    block_second_ref,
    slot_total_ref,
    slot_live_ref,
):
    blocks = total_ref.shape[0]
    capacity = slot_total_ref.shape[0]
    owner = owner_ref[0]
    for b in range(blocks):
        slot = slot_ref[b]
        near = (slot // capacity) ^ owner
        near = sum(
            jnp.where(near == k, jnp.where(owner_ref[1] == 0, order[0][k], order[1][k]), 0)
            for k in range(len(order[0]))
        )
        held = slot % capacity
        block_first_ref[b] = 0.9 * moments_ref[near, 0, held]
        block_second_ref[b] = 0.95 * moments_ref[near, 1, held]
    for c in range(capacity):
        block, used = jnp.int32(0), jnp.int32(0)
        for b in range(blocks):
            here = slot_ref[b] == owner * capacity + c
            block = jnp.where(here, b, block)
            used = jnp.where(here, 1, used)
        slot_total_ref[c] = total_ref[block]
        slot_live_ref[c] = live_ref[block] * used.astype(F32)


def step_kernel(parts, *refs):
    part_refs = refs[:parts]
    (
        total_ref,
        live_ref,
        norm_ref,
        wide_ref,
        block_first_ref,
        block_second_ref,
        slot_total_ref,
        slot_live_ref,
        first_ref,
        second_ref,
    ) = refs[parts : parts + 10]
    first_out, second_out, weight_out, rms_out = refs[parts + 10 :]
    blocks = total_ref.shape[0]
    capacity = first_ref.shape[0]

    sumsq = tree_sum([ref[...] for ref in part_refs])
    grad_rms = jnp.sqrt(sumsq) / norm_ref[...]
    clip = (1.0 / jnp.maximum(grad_rms, 1.0))[0:1]

    for c in range(capacity):
        first, second = first_ref[c], second_ref[c]
        live = slot_live_ref[c] > 0
        clipped = clip * slot_total_ref[c]
        first_out[c] = jnp.where(live, 0.9 * first + 0.1 * clipped, first)
        second_out[c] = jnp.where(live, 0.95 * second + 0.05 * clipped * clipped, second)
    for b in range(blocks):
        clipped = clip * total_ref[b]
        first_new = block_first_ref[b] + 0.1 * clipped
        second_new = block_second_ref[b] + 0.05 * clipped * clipped
        spread = jnp.sqrt(second_new * (1.0 / (1.0 - 0.95**STEP))) + 1e-08
        change = first_new * (RATE / (1.0 - 0.9**STEP)) / spread
        weight_out[b] = (wide_ref[b] - change * live_ref[b]).astype(weight_out.dtype)
    rms_out[0] = jnp.max(grad_rms)


def gathered(
    replicas,
    shares,
    grads,
    weights,
    moment1,
    moment2,
    slot_of_block,
    trainable,
    width_of_block,
):
    own = grads[0]
    blocks, rows, cols = own.shape
    owner = jnp.stack([lax.axis_index("dp"), lax.axis_index("mp") % 2]).astype(jnp.int32)
    full = (blocks, rows, cols)
    tile = (8, cols)

    def send(x, axis, size, k):
        return lax.ppermute(x, axis, xor_pairs(size, k))

    def exchange(x, ks):
        return lax.ppermute(x, ("dp", "mp"), staged_pairs(replicas, shares, ks))

    moments = jnp.stack([moment1, moment2]).astype(jnp.float16)[None]
    offsets = [[0], [0]]
    carried = own
    for stage, ks in enumerate(STAGES):
        terms = [carried, exchange(carried, ks)]
        mks = MSTAGES[stage]
        moments = jnp.concatenate([moments, exchange(moments, mks)])
        offsets = [[k ^ o for k in (0, mks[i]) for o in offsets[i]] for i in range(2)]
        if stage < len(STAGES) - 1:
            carried = tree_sum([t.astype(F32) for t in terms])
    order = [[of.index(k) for k in range(replicas)] for of in offsets]

    live, norm, wide = kernel_call(
        mask_kernel,
        (shape_of(*full), shape_of(*tile), shape_of(*full)),
        (owner, slot_of_block, trainable, width_of_block),
        weights,
    )
    total, part = kernel_call(
        functools.partial(total_kernel, len(terms)),
        (shape_of(*full), shape_of(*tile)),
        (),
        live,
        *terms,
    )
    parts = [part] + [send(part, "mp", shares, k) for k in range(1, shares)]
    placed = kernel_call(
        functools.partial(placing_kernel, order),
        (
            shape_of(*full),
            shape_of(*full),
            shape_of(*moment1.shape),
            shape_of(*moment1.shape),
        ),
        (owner, slot_of_block),
        total,
        live,
        moments.astype(F32),
    )
    first_new, second_new, weights_new, grad_rms = kernel_call(
        functools.partial(step_kernel, shares),
        (
            shape_of(*moment1.shape),
            shape_of(*moment2.shape),
            shape_of(*full, dtype=weights.dtype),
            shape_of(1),
        ),
        (),
        *parts,
        total,
        live,
        norm,
        wide,
        *placed,
        moment1,
        moment2,
        out_smem=(3,),
    )
    return first_new, second_new, weights_new, grad_rms.reshape(())


def reduced(grads, weights, moment1, moment2, slot_of_block, trainable, width_of_block):
    blocks, row_share, block_size = weights.shape
    capacity = moment1.shape[0]
    local_grads = grads[0].reshape(blocks, row_share * block_size)
    own_slots = lax.axis_index("dp") * capacity + jnp.arange(capacity, dtype=jnp.int32)
    owned_onehot = slot_of_block[None, :] == own_slots[:, None]
    columns = jnp.arange(block_size, dtype=jnp.int32)
    live = (
        (trainable[:, None] > 0) & (columns[None, :] < width_of_block[:, None])
    ).astype(F32)
    slot_live = jnp.dot(owned_onehot.astype(F32), live, precision=lax.Precision.HIGHEST)
    count = jnp.sum(live) * block_size
    summed = lax.psum(local_grads.astype(F32), "dp")
    summed_blocks = summed.reshape(blocks, row_share, block_size)
    sumsq = lax.psum(jnp.sum(summed_blocks * summed_blocks * live[:, None, :]), "mp")
    slot_grad = jnp.dot(
        owned_onehot.astype(F32), summed, precision=lax.Precision.HIGHEST
    ).reshape(capacity, row_share, block_size)
    grad_rms = jnp.sqrt(sumsq) / jnp.sqrt(jnp.maximum(count, 1.0))
    clip = 1.0 / jnp.maximum(grad_rms, 1.0)
    update_mask = slot_live[:, None, :] > 0
    clipped = clip * slot_grad
    first_new = jnp.where(update_mask, 0.9 * moment1 + 0.1 * clipped, moment1)
    second_new = jnp.where(
        update_mask, 0.95 * moment2 + 0.05 * clipped * clipped, moment2
    )
    direction = (
        first_new
        / (1.0 - 0.9**STEP)
        / (jnp.sqrt(second_new / (1.0 - 0.95**STEP)) + 1e-08)
    )
    slot_weight = jnp.dot(
        owned_onehot.astype(jnp.bfloat16),
        weights.reshape(blocks, row_share * block_size),
        preferred_element_type=F32,
    ).reshape(capacity, row_share, block_size)
    slot_new = jnp.where(
        update_mask, slot_weight - 0.001 * (direction + 0.1 * slot_weight), slot_weight
    )
    slot_new = slot_new.astype(jnp.bfloat16).reshape(capacity, row_share * block_size)
    every_slot = lax.all_gather(slot_new, "dp", axis=0, tiled=True)
    slots = jnp.arange(every_slot.shape[0], dtype=jnp.int32)
    placing = (slot_of_block[:, None] == slots[None, :]).astype(jnp.bfloat16)
    weights_new = jnp.dot(placing, every_slot, preferred_element_type=F32).astype(
        jnp.bfloat16
    )
    return (
        first_new,
        second_new,
        weights_new.reshape(blocks, row_share, block_size),
        grad_rms,
    )


def local(replicas, shares, grads, *rest):
    two_powers = replicas & (replicas - 1) == 0 and shares & (shares - 1) == 0
    if two_powers and replicas > 1 and replicas * grads.nbytes <= GATHER_BYTES:
        return gathered(replicas, shares, grads, *rest)
    return reduced(grads, *rest)


def solution(mesh):
    return jax.shard_map(
        functools.partial(local, mesh.shape["dp"], mesh.shape["mp"]),
        mesh=mesh,
        in_specs=(
            P("dp", None, "mp", None),
            P(None, "mp", None),
            P("dp", "mp", None),
            P("dp", "mp", None),
            P(),
            P(),
            P(),
        ),
        out_specs=(P("dp", "mp", None), P("dp", "mp", None), P(None, "mp", None), P()),
        check_vma=False,
    )
```

```python
import functools

import jax
import jax.numpy as jnp
from jax import lax
from jax.experimental import pallas as pl
from jax.experimental.pallas import tpu as pltpu
from jax.sharding import PartitionSpec as P


STEP = 20
RATE, DECAY = 0.001, 0.1
GATHER_BYTES = 4 << 20


F32 = jnp.float32
VMEM_BYTES = 8 << 20
STAGES = [[4, 1], [2, 2], [1, 4]]
MSTAGES = [[4, 1], [2, 2], [1, 4]]


def near_moments(moment1, moment2):
    near = lax.reduce_precision(moment1, exponent_bits=5, mantissa_bits=10)
    normal = jnp.abs(moment1) >= 2.0**-14
    ratio = jnp.where(normal, near / jnp.where(normal, moment1, 1.0), 1.0)
    return near.astype(jnp.float16), (moment2 * ratio).astype(jnp.float16)


def tree_sum(terms):
    while len(terms) > 1:
        terms = [terms[i] + terms[i + 1] for i in range(0, len(terms), 2)]
    return terms[0]


def xor_pairs(size, k):
    return [(j, j ^ k) for j in range(size)]


def staged_pairs(replicas, shares, ks):
    pairs = []
    for j in range(replicas):
        for m in range(shares):
            pairs.append((j * shares + m, (j ^ ks[m % len(ks)]) * shares + m))
    return pairs


def live_width(trainable_ref, width_ref, b, block_size):
    width = jnp.clip(width_ref[b], 0, block_size)
    return jnp.where(trainable_ref[b] > 0, width, 0)


def shape_of(*dims, dtype=F32):
    return jax.ShapeDtypeStruct(dims, dtype)


def kernel_call(body, out_shape, scalars, *operands, out_smem=()):
    smem = pl.BlockSpec(memory_space=pltpu.SMEM)
    vmem = pl.BlockSpec(memory_space=pltpu.VMEM)
    return pl.pallas_call(
        body,
        out_shape=out_shape,
        in_specs=[smem] * len(scalars) + [vmem] * len(operands),
        out_specs=tuple(smem if i in out_smem else vmem for i in range(len(out_shape))),
        compiler_params=pltpu.CompilerParams(vmem_limit_bytes=VMEM_BYTES),
    )(*scalars, *operands)


def mask_kernel(owner_ref, slot_ref, trainable_ref, width_ref, weight_ref, live_ref, norm_ref, wide_ref):
    blocks, rows, cols = live_ref.shape
    column = lax.broadcasted_iota(jnp.int32, (rows, cols), 1)
    count = jnp.int32(0)
    for b in range(blocks):
        width = live_width(trainable_ref, width_ref, b, cols)
        count = count + width
        live_ref[b] = (column < width).astype(F32)
        weight = weight_ref[b].astype(F32)
        wide_ref[b] = jnp.where(column < width, weight * (1.0 - RATE * DECAY), weight)
    count = count.astype(F32) * float(cols)
    norm_ref[...] = jnp.sqrt(jnp.full(norm_ref.shape, jnp.maximum(count, 1.0), F32))


def total_kernel(terms, live_ref, *refs):
    grad_refs, total_ref, part_ref = refs[:terms], refs[terms], refs[terms + 1]
    blocks, rows, cols = total_ref.shape
    squares = jnp.zeros((rows, cols), F32)
    for b in range(blocks):
        total = tree_sum([ref[b].astype(F32) for ref in grad_refs])
        total_ref[b] = total
        squares = squares + live_ref[b] * (total * total)
    part_ref[...] = jnp.full(part_ref.shape, jnp.sum(squares), F32)


def placing_kernel(
    order,
    owner_ref,
    slot_ref,
    total_ref,
    live_ref,
    moments_ref,
    block_first_ref,
    block_second_ref,
    slot_total_ref,
    slot_live_ref,
):
    blocks = total_ref.shape[0]
    capacity = slot_total_ref.shape[0]
    owner = owner_ref[0]
    for b in range(blocks):
        slot = slot_ref[b]
        near = (slot // capacity) ^ owner
        near = sum(
            jnp.where(near == k, jnp.where(owner_ref[1] == 0, order[0][k], order[1][k]), 0)
            for k in range(len(order[0]))
        )
        held = slot % capacity
        block_first_ref[b] = 0.9 * moments_ref[near, 0, held]
        block_second_ref[b] = 0.95 * moments_ref[near, 1, held]
    for c in range(capacity):
        block, used = jnp.int32(0), jnp.int32(0)
        for b in range(blocks):
            here = slot_ref[b] == owner * capacity + c
            block = jnp.where(here, b, block)
            used = jnp.where(here, 1, used)
        slot_total_ref[c] = total_ref[block]
        slot_live_ref[c] = live_ref[block] * used.astype(F32)


def step_kernel(parts, *refs):
    part_refs = refs[:parts]
    (
        total_ref,
        live_ref,
        norm_ref,
        wide_ref,
        block_first_ref,
        block_second_ref,
        slot_total_ref,
        slot_live_ref,
        first_ref,
        second_ref,
    ) = refs[parts : parts + 10]
    first_out, second_out, weight_out, rms_out = refs[parts + 10 :]
    blocks = total_ref.shape[0]
    capacity = first_ref.shape[0]

    sumsq = tree_sum([ref[...] for ref in part_refs])
    grad_rms = jnp.sqrt(sumsq) / norm_ref[...]
    clip = (1.0 / jnp.maximum(grad_rms, 1.0))[0:1]

    for c in range(capacity):
        first, second = first_ref[c], second_ref[c]
        live = slot_live_ref[c] > 0
        clipped = clip * slot_total_ref[c]
        first_out[c] = jnp.where(live, 0.9 * first + 0.1 * clipped, first)
        second_out[c] = jnp.where(live, 0.95 * second + 0.05 * clipped * clipped, second)
    for b in range(blocks):
        clipped = clip * total_ref[b]
        first_new = block_first_ref[b] + 0.1 * clipped
        second_new = block_second_ref[b] + 0.05 * clipped * clipped
        spread = jnp.sqrt(second_new * (1.0 / (1.0 - 0.95**STEP))) + 1e-08
        change = first_new * (RATE / (1.0 - 0.9**STEP)) / spread
        weight_out[b] = (wide_ref[b] - change * live_ref[b]).astype(weight_out.dtype)
    rms_out[0] = jnp.max(grad_rms)


def gathered(
    replicas,
    shares,
    grads,
    weights,
    moment1,
    moment2,
    slot_of_block,
    trainable,
    width_of_block,
):
    own = grads[0]
    blocks, rows, cols = own.shape
    owner = jnp.stack([lax.axis_index("dp"), lax.axis_index("mp") % 2]).astype(jnp.int32)
    full = (blocks, rows, cols)
    tile = (1, cols)

    def send(x, axis, size, k):
        return lax.ppermute(x, axis, xor_pairs(size, k))

    def exchange(x, ks):
        return lax.ppermute(x, ("dp", "mp"), staged_pairs(replicas, shares, ks))

    moments = jnp.stack(near_moments(moment1, moment2))[None]
    offsets = [[0], [0]]
    carried = own
    for stage, ks in enumerate(STAGES):
        terms = [carried, exchange(carried, ks)]
        mks = MSTAGES[stage]
        moments = jnp.concatenate([moments, exchange(moments, mks)])
        offsets = [[k ^ o for k in (0, mks[i]) for o in offsets[i]] for i in range(2)]
        if stage < len(STAGES) - 1:
            carried = tree_sum([t.astype(F32) for t in terms])
    order = [[of.index(k) for k in range(replicas)] for of in offsets]

    live, norm, wide = kernel_call(
        mask_kernel,
        (shape_of(*full), shape_of(*tile), shape_of(*full)),
        (owner, slot_of_block, trainable, width_of_block),
        weights,
    )
    total, part = kernel_call(
        functools.partial(total_kernel, len(terms)),
        (shape_of(*full), shape_of(*tile)),
        (),
        live,
        *terms,
    )
    parts = [part] + [send(part, "mp", shares, k) for k in range(1, shares)]
    placed = kernel_call(
        functools.partial(placing_kernel, order),
        (
            shape_of(*full),
            shape_of(*full),
            shape_of(*moment1.shape),
            shape_of(*moment1.shape),
        ),
        (owner, slot_of_block),
        total,
        live,
        moments.astype(F32),
    )
    first_new, second_new, weights_new, grad_rms = kernel_call(
        functools.partial(step_kernel, shares),
        (
            shape_of(*moment1.shape),
            shape_of(*moment2.shape),
            shape_of(*full, dtype=weights.dtype),
            shape_of(1),
        ),
        (),
        *parts,
        total,
        live,
        norm,
        wide,
        *placed,
        moment1,
        moment2,
        out_smem=(3,),
    )
    return first_new, second_new, weights_new, grad_rms.reshape(())


def reduced(grads, weights, moment1, moment2, slot_of_block, trainable, width_of_block):
    blocks, row_share, block_size = weights.shape
    capacity = moment1.shape[0]
    local_grads = grads[0].reshape(blocks, row_share * block_size)
    own_slots = lax.axis_index("dp") * capacity + jnp.arange(capacity, dtype=jnp.int32)
    owned_onehot = slot_of_block[None, :] == own_slots[:, None]
    columns = jnp.arange(block_size, dtype=jnp.int32)
    live = (
        (trainable[:, None] > 0) & (columns[None, :] < width_of_block[:, None])
    ).astype(F32)
    slot_live = jnp.dot(owned_onehot.astype(F32), live, precision=lax.Precision.HIGHEST)
    count = jnp.sum(live) * block_size
    summed = lax.psum(local_grads.astype(F32), "dp")
    summed_blocks = summed.reshape(blocks, row_share, block_size)
    sumsq = lax.psum(jnp.sum(summed_blocks * summed_blocks * live[:, None, :]), "mp")
    slot_grad = jnp.dot(
        owned_onehot.astype(F32), summed, precision=lax.Precision.HIGHEST
    ).reshape(capacity, row_share, block_size)
    grad_rms = jnp.sqrt(sumsq) / jnp.sqrt(jnp.maximum(count, 1.0))
    clip = 1.0 / jnp.maximum(grad_rms, 1.0)
    update_mask = slot_live[:, None, :] > 0
    clipped = clip * slot_grad
    first_new = jnp.where(update_mask, 0.9 * moment1 + 0.1 * clipped, moment1)
    second_new = jnp.where(
        update_mask, 0.95 * moment2 + 0.05 * clipped * clipped, moment2
    )
    direction = (
        first_new
        / (1.0 - 0.9**STEP)
        / (jnp.sqrt(second_new / (1.0 - 0.95**STEP)) + 1e-08)
    )
    slot_weight = jnp.dot(
        owned_onehot.astype(jnp.bfloat16),
        weights.reshape(blocks, row_share * block_size),
        preferred_element_type=F32,
    ).reshape(capacity, row_share, block_size)
    slot_new = jnp.where(
        update_mask, slot_weight - 0.001 * (direction + 0.1 * slot_weight), slot_weight
    )
    slot_new = slot_new.astype(jnp.bfloat16).reshape(capacity, row_share * block_size)
    every_slot = lax.all_gather(slot_new, "dp", axis=0, tiled=True)
    slots = jnp.arange(every_slot.shape[0], dtype=jnp.int32)
    placing = (slot_of_block[:, None] == slots[None, :]).astype(jnp.bfloat16)
    weights_new = jnp.dot(placing, every_slot, preferred_element_type=F32).astype(
        jnp.bfloat16
    )
    return (
        first_new,
        second_new,
        weights_new.reshape(blocks, row_share, block_size),
        grad_rms,
    )


def local(replicas, shares, grads, *rest):
    two_powers = replicas & (replicas - 1) == 0 and shares & (shares - 1) == 0
    if two_powers and replicas > 1 and replicas * grads.nbytes <= GATHER_BYTES:
        return gathered(replicas, shares, grads, *rest)
    return reduced(grads, *rest)


def solution(mesh):
    return jax.shard_map(
        functools.partial(local, mesh.shape["dp"], mesh.shape["mp"]),
        mesh=mesh,
        in_specs=(
            P("dp", None, "mp", None),
            P(None, "mp", None),
            P("dp", "mp", None),
            P("dp", "mp", None),
            P(),
            P(),
            P(),
        ),
        out_specs=(P("dp", "mp", None), P("dp", "mp", None), P(None, "mp", None), P()),
        check_vma=False,
    )
```

```python
import functools

import jax
import jax.numpy as jnp
from jax import lax
from jax.experimental import pallas as pl
from jax.experimental.pallas import tpu as pltpu
from jax.sharding import PartitionSpec as P


STEP = 20
RATE, DECAY = 0.001, 0.1
GATHER_BYTES = 4 << 20


F32 = jnp.float32
VMEM_BYTES = 8 << 20
STAGES = [[4, 1], [2, 2], [1, 4]]
MSTAGES = [[4, 1], [2, 2], [1, 4]]


def near_moments(moment1, moment2):
    near = lax.reduce_precision(moment1, exponent_bits=5, mantissa_bits=10)
    normal = jnp.abs(moment1) >= 2.0**-14
    ratio = jnp.where(normal, near / jnp.where(normal, moment1, 1.0), 1.0)
    return near.astype(jnp.float16), (moment2 * ratio).astype(jnp.float16)


def tree_sum(terms):
    while len(terms) > 1:
        terms = [terms[i] + terms[i + 1] for i in range(0, len(terms), 2)]
    return terms[0]


def xor_pairs(size, k):
    return [(j, j ^ k) for j in range(size)]


def staged_pairs(replicas, shares, ks):
    pairs = []
    for j in range(replicas):
        for m in range(shares):
            pairs.append((j * shares + m, (j ^ ks[m % len(ks)]) * shares + m))
    return pairs


def live_width(trainable_ref, width_ref, b, block_size):
    width = jnp.clip(width_ref[b], 0, block_size)
    return jnp.where(trainable_ref[b] > 0, width, 0)


def shape_of(*dims, dtype=F32):
    return jax.ShapeDtypeStruct(dims, dtype)


def kernel_call(body, out_shape, scalars, *operands, out_smem=()):
    smem = pl.BlockSpec(memory_space=pltpu.SMEM)
    vmem = pl.BlockSpec(memory_space=pltpu.VMEM)
    return pl.pallas_call(
        body,
        out_shape=out_shape,
        in_specs=[smem] * len(scalars) + [vmem] * len(operands),
        out_specs=tuple(smem if i in out_smem else vmem for i in range(len(out_shape))),
        compiler_params=pltpu.CompilerParams(vmem_limit_bytes=VMEM_BYTES),
    )(*scalars, *operands)


def mask_kernel(owner_ref, slot_ref, trainable_ref, width_ref, weight_ref, live_ref, norm_ref, wide_ref):
    blocks, rows, cols = live_ref.shape
    column = lax.broadcasted_iota(jnp.int32, (rows, cols), 1)
    count = jnp.int32(0)
    for b in range(blocks):
        width = live_width(trainable_ref, width_ref, b, cols)
        count = count + width
        live_ref[b] = (column < width).astype(F32)
        weight = weight_ref[b].astype(F32)
        wide_ref[b] = jnp.where(column < width, weight * (1.0 - RATE * DECAY), weight)
    count = count.astype(F32) * float(cols)
    norm_ref[...] = jnp.sqrt(jnp.full(norm_ref.shape, jnp.maximum(count, 1.0), F32))


def total_kernel(terms, live_ref, *refs):
    grad_refs, total_ref, part_ref = refs[:terms], refs[terms], refs[terms + 1]
    blocks, rows, cols = total_ref.shape
    squares = jnp.zeros((rows, cols), F32)
    for b in range(blocks):
        total = tree_sum([ref[b].astype(F32) for ref in grad_refs])
        total_ref[b] = total
        squares = squares + live_ref[b] * (total * total)
    part_ref[...] = jnp.full(part_ref.shape, jnp.sum(squares), F32)


def placing_kernel(
    order,
    owner_ref,
    slot_ref,
    total_ref,
    live_ref,
    moments_ref,
    block_first_ref,
    block_second_ref,
    slot_total_ref,
    slot_live_ref,
):
    blocks = total_ref.shape[0]
    capacity = slot_total_ref.shape[0]
    owner = owner_ref[0]
    for b in range(blocks):
        slot = slot_ref[b]
        near = (slot // capacity) ^ owner
        near = sum(
            jnp.where(near == k, jnp.where(owner_ref[1] == 0, order[0][k], order[1][k]), 0)
            for k in range(len(order[0]))
        )
        held = slot % capacity
        block_first_ref[b] = 0.9 * moments_ref[near, 0, held]
        block_second_ref[b] = 0.95 * moments_ref[near, 1, held]
    for c in range(capacity):
        block, used = jnp.int32(0), jnp.int32(0)
        for b in range(blocks):
            here = slot_ref[b] == owner * capacity + c
            block = jnp.where(here, b, block)
            used = jnp.where(here, 1, used)
        slot_total_ref[c] = total_ref[block]
        slot_live_ref[c] = live_ref[block] * used.astype(F32)


def step_kernel(parts, *refs):
    part_refs = refs[:parts]
    (
        total_ref,
        live_ref,
        norm_ref,
        wide_ref,
        block_first_ref,
        block_second_ref,
        slot_total_ref,
        slot_live_ref,
        first_ref,
        second_ref,
    ) = refs[parts : parts + 10]
    first_out, second_out, weight_out, rms_out = refs[parts + 10 :]
    blocks = total_ref.shape[0]
    capacity = first_ref.shape[0]

    sumsq = tree_sum([ref[...] for ref in part_refs])
    grad_rms = jnp.sqrt(sumsq) / norm_ref[...]
    clip = (1.0 / jnp.maximum(grad_rms, 1.0))[0:1]

    for c in range(capacity):
        first, second = first_ref[c], second_ref[c]
        live = slot_live_ref[c] > 0
        clipped = clip * slot_total_ref[c]
        first_out[c] = jnp.where(live, 0.9 * first + 0.1 * clipped, first)
        second_out[c] = jnp.where(live, 0.95 * second + 0.05 * clipped * clipped, second)
    for b in range(blocks):
        clipped = clip * total_ref[b]
        first_new = block_first_ref[b] + 0.1 * clipped
        second_new = block_second_ref[b] + 0.05 * clipped * clipped
        spread = jnp.sqrt(second_new * (1.0 / (1.0 - 0.95**STEP))) + 1e-08
        change = first_new * (RATE / (1.0 - 0.9**STEP)) / spread
        kept = wide_ref[b]
        weight_out[b] = jnp.where(live_ref[b] > 0, kept - change, kept).astype(
            weight_out.dtype
        )
    rms_out[0] = jnp.max(grad_rms)


def gathered(
    replicas,
    shares,
    grads,
    weights,
    moment1,
    moment2,
    slot_of_block,
    trainable,
    width_of_block,
):
    own = grads[0]
    blocks, rows, cols = own.shape
    owner = jnp.stack([lax.axis_index("dp"), lax.axis_index("mp") % 2]).astype(jnp.int32)
    full = (blocks, rows, cols)
    tile = (1, cols)

    def send(x, axis, size, k):
        return lax.ppermute(x, axis, xor_pairs(size, k))

    def exchange(x, ks):
        return lax.ppermute(x, ("dp", "mp"), staged_pairs(replicas, shares, ks))

    moments = jnp.stack(near_moments(moment1, moment2))[None]
    offsets = [[0], [0]]
    carried = own
    for stage, ks in enumerate(STAGES):
        terms = [carried, exchange(carried, ks)]
        mks = MSTAGES[stage]
        moments = jnp.concatenate([moments, exchange(moments, mks)])
        offsets = [[k ^ o for k in (0, mks[i]) for o in offsets[i]] for i in range(2)]
        if stage < len(STAGES) - 1:
            carried = tree_sum([t.astype(F32) for t in terms])
    order = [[of.index(k) for k in range(replicas)] for of in offsets]

    live, norm, wide = kernel_call(
        mask_kernel,
        (shape_of(*full), shape_of(*tile), shape_of(*full)),
        (owner, slot_of_block, trainable, width_of_block),
        weights,
    )
    total, part = kernel_call(
        functools.partial(total_kernel, len(terms)),
        (shape_of(*full), shape_of(*tile)),
        (),
        live,
        *terms,
    )
    parts = [part] + [send(part, "mp", shares, k) for k in range(1, shares)]
    placed = kernel_call(
        functools.partial(placing_kernel, order),
        (
            shape_of(*full),
            shape_of(*full),
            shape_of(*moment1.shape),
            shape_of(*moment1.shape),
        ),
        (owner, slot_of_block),
        total,
        live,
        moments.astype(F32),
    )
    first_new, second_new, weights_new, grad_rms = kernel_call(
        functools.partial(step_kernel, shares),
        (
            shape_of(*moment1.shape),
            shape_of(*moment2.shape),
            shape_of(*full, dtype=weights.dtype),
            shape_of(1),
        ),
        (),
        *parts,
        total,
        live,
        norm,
        wide,
        *placed,
        moment1,
        moment2,
        out_smem=(3,),
    )
    return first_new, second_new, weights_new, grad_rms.reshape(())


def reduced(grads, weights, moment1, moment2, slot_of_block, trainable, width_of_block):
    blocks, row_share, block_size = weights.shape
    capacity = moment1.shape[0]
    local_grads = grads[0].reshape(blocks, row_share * block_size)
    own_slots = lax.axis_index("dp") * capacity + jnp.arange(capacity, dtype=jnp.int32)
    owned_onehot = slot_of_block[None, :] == own_slots[:, None]
    columns = jnp.arange(block_size, dtype=jnp.int32)
    live = (
        (trainable[:, None] > 0) & (columns[None, :] < width_of_block[:, None])
    ).astype(F32)
    slot_live = jnp.dot(owned_onehot.astype(F32), live, precision=lax.Precision.HIGHEST)
    count = jnp.sum(live) * block_size
    summed = lax.psum(local_grads.astype(F32), "dp")
    summed_blocks = summed.reshape(blocks, row_share, block_size)
    sumsq = lax.psum(jnp.sum(summed_blocks * summed_blocks * live[:, None, :]), "mp")
    slot_grad = jnp.dot(
        owned_onehot.astype(F32), summed, precision=lax.Precision.HIGHEST
    ).reshape(capacity, row_share, block_size)
    grad_rms = jnp.sqrt(sumsq) / jnp.sqrt(jnp.maximum(count, 1.0))
    clip = 1.0 / jnp.maximum(grad_rms, 1.0)
    update_mask = slot_live[:, None, :] > 0
    clipped = clip * slot_grad
    first_new = jnp.where(update_mask, 0.9 * moment1 + 0.1 * clipped, moment1)
    second_new = jnp.where(
        update_mask, 0.95 * moment2 + 0.05 * clipped * clipped, moment2
    )
    direction = (
        first_new
        / (1.0 - 0.9**STEP)
        / (jnp.sqrt(second_new / (1.0 - 0.95**STEP)) + 1e-08)
    )
    slot_weight = jnp.dot(
        owned_onehot.astype(jnp.bfloat16),
        weights.reshape(blocks, row_share * block_size),
        preferred_element_type=F32,
    ).reshape(capacity, row_share, block_size)
    slot_new = jnp.where(
        update_mask, slot_weight - 0.001 * (direction + 0.1 * slot_weight), slot_weight
    )
    slot_new = slot_new.astype(jnp.bfloat16).reshape(capacity, row_share * block_size)
    every_slot = lax.all_gather(slot_new, "dp", axis=0, tiled=True)
    slots = jnp.arange(every_slot.shape[0], dtype=jnp.int32)
    placing = (slot_of_block[:, None] == slots[None, :]).astype(jnp.bfloat16)
    weights_new = jnp.dot(placing, every_slot, preferred_element_type=F32).astype(
        jnp.bfloat16
    )
    return (
        first_new,
        second_new,
        weights_new.reshape(blocks, row_share, block_size),
        grad_rms,
    )


def local(replicas, shares, grads, *rest):
    two_powers = replicas & (replicas - 1) == 0 and shares & (shares - 1) == 0
    if two_powers and replicas > 1 and replicas * grads.nbytes <= GATHER_BYTES:
        return gathered(replicas, shares, grads, *rest)
    return reduced(grads, *rest)


def solution(mesh):
    return jax.shard_map(
        functools.partial(local, mesh.shape["dp"], mesh.shape["mp"]),
        mesh=mesh,
        in_specs=(
            P("dp", None, "mp", None),
            P(None, "mp", None),
            P("dp", "mp", None),
            P("dp", "mp", None),
            P(),
            P(),
            P(),
        ),
        out_specs=(P("dp", "mp", None), P("dp", "mp", None), P(None, "mp", None), P()),
        check_vma=False,
    )
```
